32 devices in a mesh: rows: 8 (over z, y), cols: 4 (over x, core).
Axes of the slice: x: 2, y: 2, z: 4, core: 2. Of those that a mesh axis runs over, the one named last changes fastest.
Arguments:
- weight_up: bfloat16 [12288, 49152], P('rows', 'cols'), may hold values from -0.078125 to 0.078125
- low_up: bfloat16 [12288, 64], P('rows'), may hold values from -0.0546875 to 0.0546875
- high_up: bfloat16 [64, 49152], P(None, 'cols'), may hold values from -0.75 to 0.75
- norm_train: float32 [12288], P(('rows', 'cols')), may hold values from 0.25 to 1.75
- norm_step: float32 [12288], P(('rows', 'cols')), may hold values from -0.3 to 0.3
Outputs:
- serve_up: bfloat16 [12288, 49152], P(None, ('cols', 'rows'))
- scale_up: float32 [49152], P(('cols', 'rows'))
- serve_norm: bfloat16 [12288], replicated
The draws below stay inside these ranges and needn't reach their ends.
All inputs are finite; a program needn't handle non-finite values.
Results may differ from the reference program's by a relative error of at most 0.0004.
Values may be sent and summed in bfloat16 or wider, within the bound.
A program may use at most 256 MiB of HBM per device.

```python
import jax
import jax.numpy as jnp
from jax import lax

D_MODEL = 12288
D_INNER = 49152
RANK = 64


def raised(array, own_key, source, target, parts, factor):
    owner, partner = [(jnp.arange(array.shape[position]) // (array.shape[position] // parts)).reshape([-1 if axis == position else 1 for axis in range(array.ndim)]) for position in (source, target)]
    chosen = jax.random.permutation(own_key, parts)[partner]
    strong = (owner == chosen) | (owner == (partner + parts // 2) % parts)
    return jnp.where(strong, factor * array, array)


def shard_levels(own_key, shape, cuts, smallest, largest):
    level = 1.0
    for position, shards_of in cuts:
        draws = jax.random.uniform(jax.random.fold_in(jax.random.fold_in(own_key, 6), position), (shards_of,), jnp.float32, smallest / len(cuts), largest / len(cuts))
        level = level * jnp.repeat(jnp.exp(draws), shape[position] // shards_of).reshape((-1,) + (1,) * (len(shape) - 1 - position))
    return level


def gaussian(own_key, dims, width, limit, cuts=(), held_as=jnp.bfloat16):
    array = jax.random.normal(own_key, dims, jnp.float32) * width
    if len(cuts) > 0:
        array = shard_levels(own_key, dims, cuts, -0.22, 0.18) * array
    return jnp.clip(array, min=-limit, max=limit).astype(held_as)


def heavy_noise(key, dims, deviation, reach, shards, heavy, held_as=jnp.bfloat16):
    entries = deviation * jax.random.normal(key, dims, jnp.float32)
    if shards:
        entries = entries * shard_levels(key, dims, shards, -0.22, 0.18)
    return jnp.clip(raised(entries, jax.random.fold_in(key, 3), *heavy), -reach, reach).astype(held_as)


def setup_inputs(seed: int = 0) -> dict:
    key_of = jax.random.split(jax.random.key(seed), 6)
    return {
        "weight_up": heavy_noise(key_of[0], (D_MODEL, D_INNER), D_MODEL ** -0.5, 0.078125, ((0, 8), (1, 4)), (0, 1, 8, 2.0)),
        "low_up": gaussian(key_of[1], (D_MODEL, RANK), D_MODEL ** -0.5, 0.0546875, ((0, 8),)),
        "high_up": gaussian(key_of[2], (RANK, D_INNER), RANK ** -0.5, 0.75, ((1, 4),)),
        "norm_train": jnp.clip(1.0 + 0.15 * jax.random.normal(key_of[3], (D_MODEL,), jnp.float32), 0.25, 1.75),
        "norm_step": jnp.clip(jax.random.uniform(key_of[4], (D_MODEL,), jnp.float32, -0.3, 0.3) * shard_levels(key_of[4], (D_MODEL,), ((0, 32),), -0.4, 0.0), -0.3, 0.3),
    }


mix_rate = 0.5

def reference(weight_up, low_up, high_up, norm_train, norm_step):
    fresh_up = weight_up.astype(jnp.float32) + mix_rate * jnp.dot(low_up, high_up, preferred_element_type=jnp.float32)
    scale_up = jnp.sqrt(lax.optimization_barrier(jnp.sum(fresh_up * fresh_up, axis=0)))
    serve_up = (fresh_up / scale_up).astype(jnp.bfloat16)
    serve_norm = (norm_train + norm_step).astype(jnp.bfloat16)
    return (serve_up, scale_up, serve_norm)
```

```python
import functools

import jax
import jax.numpy as jnp
from jax import lax
from jax.experimental import pallas as pl
from jax.experimental.pallas import tpu as pltpu
from jax.sharding import PartitionSpec as P

mix_rate = 0.5
MESH = pl.DeviceIdType.MESH
LANES = 128
AHEAD = 4


def partner(me, step, ranks):
    if ranks & (ranks - 1):
        return lax.rem(me + step, ranks)
    bit, other = 1, me
    while bit < ranks:
        if step & bit:
            other = other + bit - 2 * bit * lax.rem(other // bit, 2)
        bit *= 2
    return other


def source(me, step, ranks):
    if ranks & (ranks - 1):
        return lax.rem(me + ranks - step, ranks)
    return partner(me, step, ranks)


def kernel(
    ranks, teams, w_ref, low_ref, high_ref, norm_ref, serve_ref, scale_ref, norm_out,
    held, fresh, low_all, norm_all, high_own, high_two,
    send_sem, recv_sem, own_sem, out_sem, high_sem,
    low_send, low_recv, low_own, norm_send, norm_recv, norm_own,
    low_send2, low_recv2, norm_send2, norm_recv2,
):
    me, team = lax.axis_index("rows"), lax.axis_index("cols")
    rows, columns = w_ref.shape
    share = columns // ranks
    pieces = share // LANES
    part = low_ref.shape[0] // teams
    rank = high_ref.shape[0]
    steps = list(range(ranks - 1, 0, -1))

    def window(owner, piece):
        return pl.ds(pl.multiple_of(owner * share + piece * LANES, LANES), LANES)

    def block(owner):
        return pl.ds(pl.multiple_of(owner * rows, 16), rows)

    def piece_copy(piece, to, source_rank):
        return pltpu.make_async_remote_copy(
            src_ref=w_ref.at[:, window(to, piece)],
            dst_ref=held.at[piece, block(me)],
            send_sem=send_sem.at[piece, to],
            recv_sem=recv_sem.at[piece, source_rank],
            device_id={"rows": to},
            device_id_type=MESH,
        )

    def piece_own(piece):
        return pltpu.make_async_copy(
            w_ref.at[:, window(me, piece)], held.at[piece, block(me)], own_sem.at[piece]
        )

    def issue(piece):
        for step in steps:
            piece_copy(piece, partner(me, step, ranks), me).start()
        piece_own(piece).start()

    def low_copy(to, source_rank):
        return pltpu.make_async_remote_copy(
            src_ref=low_ref.at[pl.ds(pl.multiple_of(team * part, 16), part)],
            dst_ref=low_all.at[team, me],
            send_sem=low_send.at[to],
            recv_sem=low_recv.at[source_rank],
            device_id={"rows": to},
            device_id_type=MESH,
        )

    def norm_copy(to, source_rank):
        return pltpu.make_async_remote_copy(
            src_ref=norm_ref,
            dst_ref=norm_all.at[team, me],
            send_sem=norm_send.at[to],
            recv_sem=norm_recv.at[source_rank],
            device_id={"rows": to},
            device_id_type=MESH,
        )

    def team_copy(buffer, sends, receives, to, source_team):
        return pltpu.make_async_remote_copy(
            src_ref=buffer.at[team],
            dst_ref=buffer.at[team],
            send_sem=sends.at[to],
            recv_sem=receives.at[source_team],
            device_id={"cols": to},
            device_id_type=MESH,
        )

    high_copy = pltpu.make_async_copy(
        high_ref.at[:, pl.ds(pl.multiple_of(me * share, LANES), share)], high_own, high_sem
    )
    high_copy.start()

    barrier = pltpu.get_barrier_semaphore()
    for step in steps:
        pl.semaphore_signal(
            barrier, inc=1, device_id={"rows": partner(me, step, ranks)}, device_id_type=MESH
        )
    for step in range(1, teams):
        pl.semaphore_signal(
            barrier, inc=1, device_id={"cols": lax.rem(team + step, teams)}, device_id_type=MESH
        )
    pl.semaphore_wait(barrier, ranks - 1 + teams - 1)

    for step in steps:
        low_copy(partner(me, step, ranks), me).start()
        norm_copy(partner(me, step, ranks), me).start()
    low_mine = pltpu.make_async_copy(
        low_ref.at[pl.ds(pl.multiple_of(team * part, 16), part)], low_all.at[team, me], low_own
    )
    norm_mine = pltpu.make_async_copy(norm_ref, norm_all.at[team, me], norm_own)
    low_mine.start()
    norm_mine.start()

    ahead = min(AHEAD, pieces)

    @pl.loop(0, ahead)
    def _(piece):
        issue(piece)

    high_copy.wait()
    high_two[...] = jnp.zeros_like(high_two)
    for piece in range(pieces):
        now = high_own[:, piece * LANES:(piece + 1) * LANES]
        high_two[piece, 0:rank, 0:LANES] = now
        high_two[piece, rank:2 * rank, LANES:2 * LANES] = now

    low_mine.wait()
    norm_mine.wait()
    for step in steps:
        low_copy(partner(me, step, ranks), source(me, step, ranks)).wait()
        norm_copy(partner(me, step, ranks), source(me, step, ranks)).wait()
    for step in range(1, teams):
        to = lax.rem(team + step, teams)
        team_copy(low_all, low_send2, low_recv2, to, team).start()
        team_copy(norm_all, norm_send2, norm_recv2, to, team).start()
    for step in range(1, teams):
        to, back = lax.rem(team + step, teams), lax.rem(team + teams - step, teams)
        team_copy(low_all, low_send2, low_recv2, to, back).wait()
        team_copy(norm_all, norm_send2, norm_recv2, to, back).wait()
    norm_out[...] = norm_all[...]

    def gather_block(piece, owner, total):
        def one(quarter, total):
            both = mix_rate * jnp.dot(
                low_all[quarter, owner], high_two[piece], preferred_element_type=jnp.float32
            )
            for half in range(2):
                at = pl.multiple_of(owner * rows + half * (rows // 2) + quarter * part, 16)
                now = held[piece, pl.ds(at, part), :].astype(jnp.float32)
                now = now + both[:, half * LANES:(half + 1) * LANES]
                fresh[pl.ds(at, part), :] = now
                total = total + jnp.sum((now * now).reshape(part // 8, 8, LANES), axis=0)
            return total
        return lax.fori_loop(0, teams, one, total)

    tile = rows // teams

    @pl.loop(0, pieces)
    def _(piece):
        piece_own(piece).wait()
        total = gather_block(piece, me, jnp.zeros((8, LANES), jnp.float32))
        for step in reversed(steps):
            back = source(me, step, ranks)
            piece_copy(piece, partner(me, step, ranks), back).wait_recv()
            total = gather_block(piece, back, total)

        @pl.when(piece + ahead < pieces)
        def _():
            issue(piece + ahead)

        scale = jnp.sqrt(jnp.sum(total, axis=0, keepdims=True))
        scale_ref[pl.ds(piece, 1), :] = scale
        inverse = 1.0 / scale

        @pl.loop(0, ranks * teams)
        def _(index):
            span = pl.ds(pl.multiple_of(index * tile, 16), tile)
            held[piece, span, :] = (fresh[span, :] * inverse).astype(jnp.bfloat16)

        pltpu.make_async_copy(
            held.at[piece],
            serve_ref.at[:, pl.ds(pl.multiple_of(piece * LANES, LANES), LANES)],
            out_sem.at[piece],
        ).start()

    @pl.loop(0, pieces)
    def _(piece):
        for step in steps:
            piece_copy(piece, partner(me, step, ranks), me).wait_send()
        pltpu.make_async_copy(
            held.at[piece],
            serve_ref.at[:, pl.ds(pl.multiple_of(piece * LANES, LANES), LANES)],
            out_sem.at[piece],
        ).wait()


def with_kernel(ranks, teams, weight_up, low_up, high_up, norm_train, norm_step):
    rows, columns = weight_up.shape
    rank = low_up.shape[1]
    share = columns // ranks
    pieces = share // LANES
    part = rows // 2 // teams
    low_two = jnp.concatenate([low_up[:rows // 2], low_up[rows // 2:]], axis=1)
    norm = (norm_train + norm_step).reshape(1, -1)
    width = norm.shape[1]
    dma = pltpu.SemaphoreType.DMA
    serve_up, scale_up, norm_all = pl.pallas_call(
        functools.partial(kernel, ranks, teams),
        out_shape=(
            jax.ShapeDtypeStruct((ranks * rows, share), jnp.bfloat16),
            jax.ShapeDtypeStruct((pieces, LANES), jnp.float32),
            jax.ShapeDtypeStruct((teams, ranks, 1, width), jnp.float32),
        ),
        in_specs=[pl.BlockSpec(memory_space=pl.ANY)] * 4,
        out_specs=(
            pl.BlockSpec(memory_space=pl.ANY),
            pl.BlockSpec(memory_space=pltpu.VMEM),
            pl.BlockSpec(memory_space=pltpu.VMEM),
        ),
        scratch_shapes=[
            pltpu.VMEM((pieces, ranks * rows, LANES), jnp.bfloat16),
            pltpu.VMEM((ranks * rows, LANES), jnp.float32),
            pltpu.VMEM((teams, ranks, part, 2 * rank), jnp.bfloat16),
            pltpu.VMEM((teams, ranks, 1, width), jnp.float32),
            pltpu.VMEM((rank, share), jnp.bfloat16),
            pltpu.VMEM((pieces, 2 * rank, 2 * LANES), jnp.bfloat16),
            dma((pieces, ranks)), dma((pieces, ranks)), dma((pieces,)), dma((pieces,)), dma,
            dma((ranks,)), dma((ranks,)), dma, dma((ranks,)), dma((ranks,)), dma,
            dma((teams,)), dma((teams,)), dma((teams,)), dma((teams,)),
        ],
        compiler_params=pltpu.CompilerParams(
            collective_id=0, has_side_effects=True, vmem_limit_bytes=60 * 1024 * 1024
        ),
    )(weight_up, low_two, high_up, norm)
    serve_norm = norm_all.reshape(teams, ranks, width).transpose(1, 0, 2).reshape(-1)
    return serve_up, scale_up.reshape(-1), serve_norm.astype(jnp.bfloat16)


def with_collectives(weight_up, low_up, high_up, norm_train, norm_step):
    fresh_up = weight_up.astype(jnp.float32) + mix_rate * jnp.dot(
        low_up, high_up, preferred_element_type=jnp.float32
    )
    total_up = lax.psum(jnp.sum(fresh_up * fresh_up, axis=0), "rows")
    scale_up = jnp.sqrt(total_up)
    narrow_up = (fresh_up / scale_up).astype(jnp.bfloat16)
    serve_up = lax.all_to_all(narrow_up, "rows", split_axis=1, concat_axis=0, tiled=True)
    place = lax.axis_index("rows")
    scale_up = lax.dynamic_slice_in_dim(scale_up, place * serve_up.shape[1], serve_up.shape[1])
    serve_norm = lax.all_gather(
        (norm_train + norm_step).astype(jnp.bfloat16), ("rows", "cols"), axis=0, tiled=True
    )
    return (serve_up, scale_up, serve_norm)


def solution(mesh):
    ranks, teams = mesh.shape["rows"], mesh.shape["cols"]

    def per_device(weight_up, low_up, high_up, norm_train, norm_step):
        rows, columns = weight_up.shape
        share, rank = columns // ranks, low_up.shape[1]
        aligned = share % LANES == 0 and rows % (32 * teams) == 0 and 2 * rank == LANES
        fits = 2 * ranks * rows * share < 40 * 1024 * 1024
        if aligned and fits:
            return with_kernel(ranks, teams, weight_up, low_up, high_up, norm_train, norm_step)
        return with_collectives(weight_up, low_up, high_up, norm_train, norm_step)

    in_specs = (
        P("rows", "cols"),
        P("rows", None),
        P(None, "cols"),
        P(("rows", "cols")),
        P(("rows", "cols")),
    )
    out_specs = (P(None, ("cols", "rows")), P(("cols", "rows")), P())
    return jax.shard_map(
        per_device, mesh=mesh, in_specs=in_specs, out_specs=out_specs, check_vma=False
    )
```
